256 devices in a mesh: section: 8 (over x, core), ep: 32 (over y, z).
Axes of the slice: x: 4, y: 4, z: 8, core: 2. Of those that a mesh axis runs over, the one named last changes fastest.
Arguments:
- hidden_states: bfloat16 [1536, 6144], P('ep'), may hold values from -6 to 6
- route_experts: int32 [1536, 2], P('ep'), may hold values from 0 to 7, all different within a row; in each aligned block of 48 rows (0 to 47, 48 to 95, ...) at most 24 rows name the same one
- route_weights: float32 [1536, 2], P('ep'), may hold values from 0.05 to 1
- gate_weight: bfloat16 [32, 6144, 2048], P('ep', None, 'section'), may hold values from -0.078125 to 0.078125
- up_weight: bfloat16 [32, 6144, 2048], P('ep', None, 'section'), may hold values from -0.078125 to 0.078125
- down_weight: bfloat16 [32, 2048, 6144], P('ep', 'section'), may hold values from -0.0625 to 0.0625
Outputs:
- layer_out: bfloat16 [1536, 6144], P('ep', 'section')
The draws below stay inside these ranges and needn't reach their ends.
Inputs may be any that keep to these rules, and one draw needn't show every extreme that they name: `route_experts`: each row names two different experts. Among the 48 rows of one ep index no expert is named by more than 24 rows, and in every draw some expert is named by exactly 24 rows of some ep index.
All inputs are finite; a program needn't handle non-finite values.
Results may differ from the reference program's by a relative error of at most 0.015.
Values may be sent and summed in bfloat16 or wider, within the bound.
A program may use at most 128 MiB of HBM per device.

```python
import math
import jax
import jax.numpy as jnp
import numpy as np
from jax import lax

D = 6144
FF = 8192
EXPERTS = 8
TOK_DEV = 48
TOKENS = 1536
CAP = 24
MEMBERS = 4
N_SECTION = 8
N_EP = 32


def levels(key, extent, pieces, smallest, top_value):
    factor_of, own = 1.0, jax.random.fold_in(key, 6)
    for axis_at, blocks in pieces:
        steps = jnp.exp(jax.random.uniform(jax.random.fold_in(own, axis_at), (blocks,), jnp.float32, smallest / len(pieces), top_value / len(pieces)))
        factor_of = factor_of * jnp.repeat(steps, extent[axis_at] // blocks).reshape([-1 if axis == axis_at else 1 for axis in range(len(extent))])
    return factor_of


def routed_block(own_key, own, number, rows, count, top, most, lean):
    ranking = jax.random.permutation(own_key, count)
    packed, ordinary = portions_of(count, rows * top, most, lean, True), portions_of(count, rows * top, most, lean, False)
    places = jnp.arange(count)

    def named(sizes, turn):
        used = int((sizes > 0).sum())
        fixed = max(1, used // 4)
        passed = fixed + (places - fixed + turn * (used - fixed)) % max(1, count - fixed)
        return jnp.zeros((count,), jnp.int32).at[ranking[jnp.where(places < fixed, places, passed)]].set(jnp.asarray(sizes, jnp.int32))

    sizes = jnp.where(number % 4 == 0, named(packed, number // 4), named(ordinary, number - number // 4 - 1))
    mixed = jax.random.permutation(jax.random.fold_in(own, 3), count)
    donor, receiver = mixed[0:count // 2 * 2:2], mixed[1:count // 2 * 2:2]
    margin = jnp.minimum(sizes[donor] - 1, most - sizes[receiver]) // 2
    margin = jnp.where((donor == ranking[0]) | (receiver == ranking[0]) | (sizes[receiver] == 0), 0, jnp.maximum(margin, 0))
    passed = jax.random.randint(jax.random.fold_in(own, 4), (count // 2,), 0, 1 << 20) % (margin + 1)
    sizes = sizes.at[donor].add(-passed).at[receiver].add(passed)
    items = jnp.searchsorted(jnp.cumsum(sizes), jnp.arange(rows * top), side="right").astype(jnp.int32)
    table = items.reshape(top, rows).T
    table = table[jax.random.permutation(jax.random.fold_in(own, 1), rows)]
    turn = jax.random.randint(jax.random.fold_in(own, 2), (rows, 1), 0, top)
    return jnp.take_along_axis(table, (jnp.arange(top)[None, :] + turn) % top, axis=1)


def portions_of(amount, total, limit, lean, full):
    portions = [(1 << 20) // math.isqrt(rank ** lean) + 1 for rank in range(1, amount + 1)]
    largest = limit if full else min(limit, max(-(-total // amount), total * portions[0] // sum(portions)))
    least = 1 if total - largest >= amount - 1 else 0
    holding, spare = [largest] + [least] * (amount - 1), total - largest - least * (amount - 1)
    while spare > 0:
        candidates = [i for i in range(1, amount) if holding[i] < largest] or [i for i in range(1, amount) if holding[i] < limit]
        pool, budget = sum([portions[i] for i in candidates]), spare
        for i in candidates:
            extra = min(limit - holding[i], max(1, budget * portions[i] // pool), spare)
            holding[i] = holding[i] + extra
            spare = spare - extra
    return np.array(holding)


def gaussian(own_key, shape, spread, limit, cuts=(), held_as=jnp.bfloat16):
    drawn = spread * jax.random.normal(own_key, shape, jnp.float32)
    if cuts:
        drawn = drawn * levels(own_key, shape, cuts, -0.22, 0.18)
    return jnp.clip(drawn, -limit, limit).astype(held_as)


def setup_inputs(seed: int = 0) -> dict:
    streams_of = jax.random.split(jax.random.key(seed), 7)
    hidden_states = gaussian(streams_of[0], (TOKENS, D), 1.0, 6.0, ((0, 32),))
    route_experts_keys = jax.random.split(jax.random.fold_in(streams_of[1], 1), TOKENS // TOK_DEV)
    route_experts_turns = jax.random.permutation(jax.random.fold_in(streams_of[1], 3), TOKENS // TOK_DEV)
    route_experts = jax.vmap(lambda own, number: routed_block(jax.random.fold_in(streams_of[1], 2), own, number, TOK_DEV, EXPERTS, 2, CAP, 2))(route_experts_keys, route_experts_turns).reshape((TOKENS, 2))
    route_weights = jnp.clip(0.05 + 0.95 * jax.random.uniform(streams_of[2], (TOKENS, 2), jnp.float32) ** levels(streams_of[2], (TOKENS, 2), ((0, 32),), -0.2, 0.2), 0.05, 1.0)
    gate_weight = gaussian(streams_of[3], (N_EP, D, FF // MEMBERS), D ** -0.5, 0.078125, ((0, 32), (2, 8)))
    up_weight = gaussian(streams_of[4], (N_EP, D, FF // MEMBERS), D ** -0.5, 0.078125, ((0, 32), (2, 8)))
    down_weight = gaussian(streams_of[5], (N_EP, FF // MEMBERS, D), FF ** -0.5, 0.0625, ((0, 32), (1, 8)))
    return dict(hidden_states=hidden_states, route_experts=route_experts, route_weights=route_weights, gate_weight=gate_weight, up_weight=up_weight, down_weight=down_weight)


def shard_output(slot_rows, gate_block, up_block, down_block):
    gate_value = jnp.dot(slot_rows, gate_block, preferred_element_type=jnp.float32)
    up_value = jnp.dot(slot_rows, up_block, preferred_element_type=jnp.float32)
    hidden = (jax.nn.silu(gate_value) * up_value).astype(jnp.bfloat16)
    return jnp.dot(hidden, down_block, preferred_element_type=jnp.float32).astype(jnp.bfloat16).astype(jnp.float32)


def reference(hidden_states, route_experts, route_weights, gate_weight, up_weight, down_weight):
    members = N_EP // EXPERTS
    capacity = TOK_DEV // 2
    shard_width = gate_weight.shape[2] // N_SECTION
    blocks = route_experts.reshape(N_EP, TOK_DEV * 2)
    labels = jnp.arange(EXPERTS, dtype=jnp.int32)
    one_hot = (blocks[:, :, None] == labels[None, None, :]).astype(jnp.int32)
    earlier = jnp.cumsum(one_hot, axis=1) - one_hot
    slot_index = jnp.sum(earlier * one_hot, axis=2)
    entry = jnp.arange(TOK_DEV * 2, dtype=jnp.int32)
    token_row = jnp.arange(N_EP, dtype=jnp.int32)[:, None] * TOK_DEV + entry[None, :] // 2
    flat_weights = route_weights.reshape(N_EP, TOK_DEV * 2)
    slots = jnp.arange(capacity, dtype=jnp.int32)
    result = jnp.zeros((TOKENS, D), jnp.float32)
    for expert in range(EXPERTS):
        matches = ((blocks[:, None, :] == expert) & (slot_index[:, None, :] == slots[None, :, None])).astype(jnp.int32)
        rows_index = jnp.sum(matches * token_row[:, None, :], axis=2).reshape(-1).astype(jnp.int32)
        weight_slot = jnp.sum(matches.astype(jnp.float32) * flat_weights[:, None, :], axis=2).reshape(-1)
        gathered = hidden_states[rows_index]

        def add_shard(shard, total):
            member = shard // N_SECTION
            section_index = shard % N_SECTION
            block_index = (expert * members + member).astype(jnp.int32)
            offset = (section_index * shard_width).astype(jnp.int32)
            gate_block = lax.dynamic_slice_in_dim(lax.dynamic_index_in_dim(gate_weight, block_index, 0, keepdims=False), offset, shard_width, 1)
            up_block = lax.dynamic_slice_in_dim(lax.dynamic_index_in_dim(up_weight, block_index, 0, keepdims=False), offset, shard_width, 1)
            down_block = lax.dynamic_slice_in_dim(lax.dynamic_index_in_dim(down_weight, block_index, 0, keepdims=False), offset, shard_width, 0)
            return total + shard_output(gathered, gate_block, up_block, down_block)

        total = lax.fori_loop(0, members * N_SECTION, add_shard, jnp.zeros((N_EP * capacity, D), jnp.float32))
        result = result.at[rows_index].add(weight_slot[:, None] * total)
    return result.astype(jnp.bfloat16)
```

```python
import jax
import jax.numpy as jnp
from jax import lax
from jax.experimental import pallas as pl
from jax.experimental.pallas import tpu as pltpu
from jax.sharding import PartitionSpec as P

MESH = pl.DeviceIdType.MESH
BF16 = jnp.bfloat16
F32 = jnp.float32

NX, NY, NZ = 4, 4, 8
SECTIONS = 2 * NX
TOK = 48
CAP = 24
ROWS = NY * CAP
GROUPS = 2
MEMBERS = 4
CHUNKS = NZ
LAST = CHUNKS + 6


def distance(k):
    return jnp.where(k % 2 == 1, (k + 1) // 2, (NZ - k // 2) % NZ)


def kernel(
    hid, experts, weights, wg, wu, wd, out,
    tok, meta, oh, merged, blk, wgu, wdn, xg, part, dbuf, r0, r1, r2, zs, ret, ysend, yret,
    s_loc, s_wd, s_yt, s_ym, s_yr, s_zr, s_x0, s_x1, s_x2, s_pr, s_dr, s_r0, s_r1, s_r2, s_ret,
    s_sa, s_sr, s_sz, s_sy,
):
    feats = tok.shape[-1]
    units = wdn.shape[1]
    s = lax.axis_index("section")
    ep = lax.axis_index("ep")
    c, x = s % 2, s // 2
    y, z = ep // NZ, ep % NZ
    step = 1 - 2 * c
    xa, xb, xo = (x + step + NX) % NX, (x - step + NX) % NX, (x + 2) % NX
    to_a = {"section": 2 * xa + c, "ep": ep}
    to_b = {"section": 2 * xb + c, "ep": ep}
    to_p = {"section": 2 * x + 1 - c, "ep": ep}
    mine, theirs = c * NX, (1 - c) * NX
    me = mine + x

    def at_y(yy):
        return {"section": s, "ep": yy * NZ + z}

    def at_z(zz):
        return {"section": s, "ep": y * NZ + zz}

    def send(src, dst, ssem, rsem, to):
        return pltpu.make_async_remote_copy(
            src_ref=src, dst_ref=dst, send_sem=ssem, recv_sem=rsem, device_id=to, device_id_type=MESH
        )

    def wait(ref, sem):
        pltpu.make_async_copy(ref, ref, sem).wait()

    tok_copy = pltpu.make_async_copy(
        hid.at[:, pl.ds(pl.multiple_of(s * feats, 128), feats)], tok.at[y], s_loc.at[0]
    )
    tok_copy.start()
    g_copy = pltpu.make_async_copy(wg, wgu.at[:, :, pl.ds(0, units)], s_loc.at[1])
    u_copy = pltpu.make_async_copy(wu, wgu.at[:, :, pl.ds(units, units)], s_loc.at[2])
    g_copy.start()
    u_copy.start()
    d_copies = [
        pltpu.make_async_copy(wd.at[:, pl.ds(i * feats, feats)], wdn.at[i], s_wd.at[i])
        for i in range(SECTIONS)
    ]
    for copy in d_copies:
        copy.start()

    meta[y] = jnp.zeros((8, 128), F32)
    meta[y, pl.ds(0, 2), pl.ds(0, TOK)] = weights[...]
    meta[y, pl.ds(2, 2), pl.ds(0, TOK)] = experts[...].astype(F32)

    barrier = pltpu.get_barrier_semaphore()
    peers = [at_y((y + j) % NY) for j in range(1, NY)]
    peers += [at_z((z + d) % NZ) for d in range(1, NZ)]
    peers += [to_a, to_b, to_p]
    for peer in peers:
        pl.semaphore_signal(barrier, inc=1, device_id=peer, device_id_type=MESH)
    pl.semaphore_wait(barrier, len(peers))

    tok_copy.wait()
    for j in range(1, NY):
        to = at_y((y + j) % NY)
        send(meta.at[y], meta.at[y], s_sy.at[0], s_ym.at[j], to).start()
        send(tok.at[y], tok.at[y], s_sy.at[1], s_yt.at[j], to).start()
    for j in range(1, NY):
        wait(meta.at[0], s_ym.at[j])

    lane = lax.broadcasted_iota(jnp.int32, (TOK, 128), 1).astype(F32)
    earlier = (
        lax.broadcasted_iota(jnp.int32, (TOK, TOK), 0) > lax.broadcasted_iota(jnp.int32, (TOK, TOK), 1)
    ).astype(F32).astype(BF16)
    slot_lane = lax.broadcasted_iota(jnp.int32, (TOK, GROUPS * ROWS), 1).astype(F32)
    first_expert = (GROUPS * y).astype(F32)
    for i in range(NY):
        table = meta[i].T[:TOK]
        named = [(table[:, 2 + n : 3 + n] == lane).astype(F32) for n in range(2)]
        before = jnp.dot(earlier, (named[0] + named[1]).astype(BF16), preferred_element_type=F32)
        for n in range(2):
            group = table[:, 2 + n : 3 + n] - first_expert
            place = group * ROWS + i * CAP + jnp.sum(named[n] * before, axis=1, keepdims=True)
            here = (group >= 0.0) & (group < float(GROUPS))
            place = jnp.where(here, place, -1.0)
            oh[n, pl.ds(i * TOK, TOK), :] = (place == slot_lane).astype(F32).astype(BF16)
    for j in range(1, NY):
        wait(tok.at[0], s_yt.at[j])
    packed = lax.dot_general(
        oh[0] + oh[1], tok[...].reshape(NY * TOK, feats), (((0,), (0,)), ((), ())), preferred_element_type=F32
    ).astype(BF16)
    blk[0] = packed[:ROWS]
    blk[1] = packed[ROWS:]
    xg[0, me] = blk[z // MEMBERS]

    for k in range(1, CHUNKS):
        d = (k + 1) // 2 if k % 2 else NZ - k // 2
        zz = (z + d) % NZ
        send(blk.at[zz // MEMBERS], xg.at[k, me], s_sz.at[0], s_zr.at[k], at_z(zz)).start()

    def gather_own(k):
        @pl.when(k > 0)
        def _():
            wait(xg.at[k, me], s_zr.at[k])

        send(xg.at[k, me], xg.at[k, me], s_sa.at[k], s_x0.at[k], to_a).start()
        send(xg.at[k, me], xg.at[k, me], s_sa.at[k], s_x1.at[k], to_b).start()
        send(xg.at[k, me], xg.at[k, me], s_sa.at[k], s_pr.at[k], to_p).start()

    def gather_relay(k):
        src = mine + xb
        wait(xg.at[k, src], s_x0.at[k])
        send(xg.at[k, src], xg.at[k, src], s_sa.at[k], s_x2.at[k], to_a).start()
        send(xg.at[k, src], xg.at[k, src], s_sa.at[k], s_pr.at[k], to_p).start()

    def gather_rest(k):
        wait(xg.at[k, mine + xa], s_x1.at[k])
        send(xg.at[k, mine + xa], xg.at[k, mine + xa], s_sa.at[k], s_pr.at[k], to_p).start()
        wait(xg.at[k, mine + xo], s_x2.at[k])
        send(xg.at[k, mine + xo], xg.at[k, mine + xo], s_sa.at[k], s_pr.at[k], to_p).start()

    def compute(k):
        wait(xg.at[k, pl.ds(0, NX)], s_pr.at[k])
        both = jnp.zeros((ROWS, 2 * units), F32)
        for slot in range(SECTIONS):
            sec = 2 * (slot % NX) + slot // NX
            both = both + jnp.dot(xg[k, slot], wgu[sec], preferred_element_type=F32)
        gate, up = both[:, :units], both[:, units:]
        hidden = (gate / (1.0 + jnp.exp(-gate)) * up).astype(BF16)
        for i in range(NX):
            part[k, theirs + i] = jnp.dot(hidden, wdn[2 * i + 1 - c], preferred_element_type=F32).astype(BF16)
        for i in range(NX):
            part[k, mine + i] = jnp.dot(hidden, wdn[2 * i + c], preferred_element_type=F32).astype(BF16)
            send(part.at[k, theirs + i], dbuf.at[k, i], s_sr.at[k], s_dr.at[k], to_p).start()

    def pair_sum(k, xx):
        return part[k, mine + xx].astype(F32) + dbuf[k, xx].astype(F32)

    def reduce_first(k):
        wait(dbuf.at[k], s_dr.at[k])
        part[k, mine + xo] = pair_sum(k, xo).astype(BF16)
        part[k, mine + xb] = pair_sum(k, xb).astype(BF16)
        send(part.at[k, mine + xo], r0.at[k], s_sr.at[k], s_r0.at[k], to_a).start()
        send(part.at[k, mine + xb], r1.at[k], s_sr.at[k], s_r1.at[k], to_b).start()

    def reduce_relay(k):
        wait(r0.at[k], s_r0.at[k])
        part[k, mine + xa] = (pair_sum(k, xa) + r0[k].astype(F32)).astype(BF16)
        send(part.at[k, mine + xa], r2.at[k], s_sr.at[k], s_r2.at[k], to_a).start()

    def reduce_last(k):
        wait(r1.at[k], s_r1.at[k])
        wait(r2.at[k], s_r2.at[k])
        total = (pair_sum(k, x) + (r1[k].astype(F32) + r2[k].astype(F32))).astype(BF16)
        zs[k] = total

        @pl.when(k == 0)
        def _():
            ret[0] = total

        @pl.when(k > 0)
        def _():
            d = distance(k)
            send(zs.at[k], ret.at[d], s_sz.at[1], s_ret.at[d], at_z((z - d + NZ) % NZ)).start()

    def turn(k, _):
        def stage(f, lag):
            @pl.when((k >= lag) & (k < CHUNKS + lag))
            def _():
                f(k - lag)

        stage(gather_own, 0)
        stage(gather_relay, 1)
        stage(gather_rest, 2)
        stage(reduce_relay, 5)
        stage(reduce_last, 6)
        stage(reduce_first, 4)

        @pl.when(k == 3)
        def _():
            g_copy.wait()
            u_copy.wait()
            for copy in d_copies:
                copy.wait()

        stage(compute, 3)
        return 0

    lax.fori_loop(0, LAST, turn, 0)

    for d in range(1, NZ):
        wait(ret.at[d], s_ret.at[d])
    for g in range(GROUPS):
        total = jnp.zeros((ROWS, feats), F32)
        for m in range(MEMBERS):
            total = total + ret[(MEMBERS * g + m - z + NZ) % NZ].astype(F32)
        merged[pl.ds(g * ROWS, ROWS), :] = total.astype(BF16)
    summed = merged[...]
    for i in range(NY):
        table = meta[i].T[:TOK]
        first = jnp.dot(oh[0, pl.ds(i * TOK, TOK), :], summed, preferred_element_type=F32)
        second = jnp.dot(oh[1, pl.ds(i * TOK, TOK), :], summed, preferred_element_type=F32)
        ysend[i] = (table[:, 0:1] * first + table[:, 1:2] * second).astype(BF16)
    for j in range(1, NY):
        yy = (y + j) % NY
        send(ysend.at[yy], yret.at[j], s_sy.at[2], s_yr.at[j], at_y(yy)).start()
    total = ysend[y].astype(F32)
    for j in range(1, NY):
        wait(yret.at[j], s_yr.at[j])
        total = total + yret[j].astype(F32)
    out[...] = total.astype(BF16)

    for k in range(CHUNKS):
        wait(xg.at[k, pl.ds(0, 7)], s_sa.at[k])
        wait(part.at[k, pl.ds(0, 7)], s_sr.at[k])
    wait(zs.at[pl.ds(0, 7)], s_sz.at[0])
    wait(zs.at[pl.ds(0, 7)], s_sz.at[1])
    wait(meta.at[pl.ds(0, 3)], s_sy.at[0])
    wait(tok.at[pl.ds(0, 3)], s_sy.at[1])
    wait(tok.at[pl.ds(0, 3)], s_sy.at[2])


def on_device(hidden_states, route_experts, route_weights, gate_weight, up_weight, down_weight):
    width = hidden_states.shape[1]
    units = gate_weight.shape[2]
    feats = width // SECTIONS
    dma = pltpu.SemaphoreType.DMA
    block = (ROWS, feats)
    return pl.pallas_call(
        kernel,
        out_shape=jax.ShapeDtypeStruct((TOK, feats), BF16),
        in_specs=[
            pl.BlockSpec(memory_space=pl.ANY),
            pl.BlockSpec(memory_space=pltpu.VMEM),
            pl.BlockSpec(memory_space=pltpu.VMEM),
            *[pl.BlockSpec(memory_space=pl.ANY)] * 3,
        ],
        out_specs=pl.BlockSpec(memory_space=pltpu.VMEM),
        scratch_shapes=[
            pltpu.VMEM((NY, TOK, feats), BF16),
            pltpu.VMEM((NY, 8, 128), F32),
            pltpu.VMEM((2, NY * TOK, GROUPS * ROWS), BF16),
            pltpu.VMEM((GROUPS * ROWS, feats), BF16),
            pltpu.VMEM((GROUPS, *block), BF16),
            pltpu.VMEM((SECTIONS, feats, 2 * units), BF16),
            pltpu.VMEM((SECTIONS, units, feats), BF16),
            pltpu.VMEM((CHUNKS, SECTIONS, *block), BF16),
            pltpu.VMEM((CHUNKS, SECTIONS, *block), BF16),
            pltpu.VMEM((CHUNKS, NX, *block), BF16),
            pltpu.VMEM((CHUNKS, *block), BF16),
            pltpu.VMEM((CHUNKS, *block), BF16),
            pltpu.VMEM((CHUNKS, *block), BF16),
            pltpu.VMEM((CHUNKS, *block), BF16),
            pltpu.VMEM((CHUNKS, *block), BF16),
            pltpu.VMEM((NY, TOK, feats), BF16),
            pltpu.VMEM((NY, TOK, feats), BF16),
            dma((3,)),
            dma((SECTIONS,)),
            *[dma((NY,))] * 3,
            *[dma((CHUNKS,))] * 10,
            dma((CHUNKS,)),
            dma((CHUNKS,)),
            dma((2,)),
            dma((3,)),
        ],
        compiler_params=pltpu.CompilerParams(
            collective_id=0, has_side_effects=True, vmem_limit_bytes=60 * 1024 * 1024
        ),
    )(
        hidden_states,
        route_experts.T,
        route_weights.T,
        gate_weight.reshape(SECTIONS, feats, units),
        up_weight.reshape(SECTIONS, feats, units),
        down_weight.reshape(units, width),
    )


def solution(mesh):
    return jax.shard_map(
        on_device,
        mesh=mesh,
        in_specs=(
            P("ep", None),
            P("ep", None),
            P("ep", None),
            P("ep", None, "section"),
            P("ep", None, "section"),
            P("ep", "section", None),
        ),
        out_specs=P("ep", "section"),
        check_vma=False,
    )
```

```python
import jax
import jax.numpy as jnp
from jax import lax
from jax.experimental import pallas as pl
from jax.experimental.pallas import tpu as pltpu
from jax.sharding import PartitionSpec as P

MESH = pl.DeviceIdType.MESH
BF16 = jnp.bfloat16
F32 = jnp.float32

NX, NY, NZ = 4, 4, 8
SECTIONS = 2 * NX
TOK = 48
CAP = 24
ROWS = NY * CAP
GROUPS = 2
MEMBERS = 4
CHUNKS = NZ
LAST = CHUNKS + 9


def distance(k):
    return jnp.where(k % 2 == 1, (k + 1) // 2, (NZ - k // 2) % NZ)


def reduce_order(q):
    return jnp.where(q < 5, q + 3, jnp.where(q == 7, 0, q - 4))


def kernel(
    hid, experts, weights, wg, wu, wd, out,
    tok, meta, oh, merged, blk, wgu, wdn, xg, part, dbuf, r0, r1, r2, zs, ret, ysend, yret,
    s_loc, s_wd, s_yt, s_ym, s_yr, s_zr, s_x0, s_x1, s_x2, s_pr, s_dr, s_r0, s_r1, s_r2, s_ret,
    s_sa, s_sr, s_sz, s_sy,
):
    feats = tok.shape[-1]
    units = wdn.shape[1]
    s = lax.axis_index("section")
    ep = lax.axis_index("ep")
    c, x = s % 2, s // 2
    y, z = ep // NZ, ep % NZ
    step = 1 - 2 * c
    xa, xb, xo = (x + step + NX) % NX, (x - step + NX) % NX, (x + 2) % NX
    to_a = {"section": 2 * xa + c, "ep": ep}
    to_b = {"section": 2 * xb + c, "ep": ep}
    to_p = {"section": 2 * x + 1 - c, "ep": ep}
    mine, theirs = c * NX, (1 - c) * NX
    me = mine + x

    def at_y(yy):
        return {"section": s, "ep": yy * NZ + z}

    def at_z(zz):
        return {"section": s, "ep": y * NZ + zz}

    def send(src, dst, ssem, rsem, to):
        return pltpu.make_async_remote_copy(
            src_ref=src, dst_ref=dst, send_sem=ssem, recv_sem=rsem, device_id=to, device_id_type=MESH
        )

    def wait(ref, sem):
        pltpu.make_async_copy(ref, ref, sem).wait()

    tok_copy = pltpu.make_async_copy(
        hid.at[:, pl.ds(pl.multiple_of(s * feats, 128), feats)], tok.at[y], s_loc.at[0]
    )
    tok_copy.start()
    g_copy = pltpu.make_async_copy(wg, wgu.at[:, :, pl.ds(0, units)], s_loc.at[1])
    u_copy = pltpu.make_async_copy(wu, wgu.at[:, :, pl.ds(units, units)], s_loc.at[2])
    g_copy.start()
    u_copy.start()
    d_copies = [
        pltpu.make_async_copy(wd.at[:, pl.ds(i * feats, feats)], wdn.at[i], s_wd.at[i])
        for i in range(SECTIONS)
    ]
    for copy in d_copies:
        copy.start()

    meta[y] = jnp.zeros((8, 128), F32)
    meta[y, pl.ds(0, 2), pl.ds(0, TOK)] = weights[...]
    meta[y, pl.ds(2, 2), pl.ds(0, TOK)] = experts[...].astype(F32)

    barrier = pltpu.get_barrier_semaphore()
    peers = [at_y((y + j) % NY) for j in range(1, NY)]
    peers += [at_z((z + d) % NZ) for d in range(1, NZ)]
    peers += [to_a, to_b, to_p]
    for peer in peers:
        pl.semaphore_signal(barrier, inc=1, device_id=peer, device_id_type=MESH)
    pl.semaphore_wait(barrier, len(peers))

    tok_copy.wait()
    for j in range(1, NY):
        to = at_y((y + j) % NY)
        send(meta.at[y], meta.at[y], s_sy.at[0], s_ym.at[j], to).start()
        send(tok.at[y], tok.at[y], s_sy.at[1], s_yt.at[j], to).start()
    for j in range(1, NY):
        wait(meta.at[0], s_ym.at[j])

    lane = lax.broadcasted_iota(jnp.int32, (TOK, 128), 1).astype(F32)
    earlier = (
        lax.broadcasted_iota(jnp.int32, (TOK, TOK), 0) > lax.broadcasted_iota(jnp.int32, (TOK, TOK), 1)
    ).astype(F32).astype(BF16)
    slot_lane = lax.broadcasted_iota(jnp.int32, (TOK, GROUPS * ROWS), 1).astype(F32)
    first_expert = (GROUPS * y).astype(F32)
    for i in range(NY):
        table = meta[i].T[:TOK]
        named = [(table[:, 2 + n : 3 + n] == lane).astype(F32) for n in range(2)]
        before = jnp.dot(earlier, (named[0] + named[1]).astype(BF16), preferred_element_type=F32)
        for n in range(2):
            group = table[:, 2 + n : 3 + n] - first_expert
            place = group * ROWS + i * CAP + jnp.sum(named[n] * before, axis=1, keepdims=True)
            here = (group >= 0.0) & (group < float(GROUPS))
            place = jnp.where(here, place, -1.0)
            oh[n, pl.ds(i * TOK, TOK), :] = (place == slot_lane).astype(F32).astype(BF16)
    for j in range(1, NY):
        wait(tok.at[0], s_yt.at[j])
    packed = lax.dot_general(
        oh[0] + oh[1], tok[...].reshape(NY * TOK, feats), (((0,), (0,)), ((), ())), preferred_element_type=F32
    ).astype(BF16)
    blk[0] = packed[:ROWS]
    blk[1] = packed[ROWS:]
    xg[0, me] = blk[z // MEMBERS]

    for k in range(1, CHUNKS):
        d = (k + 1) // 2 if k % 2 else NZ - k // 2
        zz = (z + d) % NZ
        send(blk.at[zz // MEMBERS], xg.at[k, me], s_sz.at[0], s_zr.at[k], at_z(zz)).start()

    def gather_own(k):
        @pl.when(k > 0)
        def _():
            wait(xg.at[k, me], s_zr.at[k])

        send(xg.at[k, me], xg.at[k, me], s_sa.at[k], s_x0.at[k], to_a).start()
        send(xg.at[k, me], xg.at[k, me], s_sa.at[k], s_x1.at[k], to_b).start()
        send(xg.at[k, me], xg.at[k, me], s_sa.at[k], s_pr.at[k], to_p).start()

    def gather_relay(k):
        src = mine + xb
        wait(xg.at[k, src], s_x0.at[k])
        send(xg.at[k, src], xg.at[k, src], s_sa.at[k], s_x2.at[k], to_a).start()
        send(xg.at[k, src], xg.at[k, src], s_sa.at[k], s_pr.at[k], to_p).start()

    def gather_rest(k):
        wait(xg.at[k, mine + xa], s_x1.at[k])
        send(xg.at[k, mine + xa], xg.at[k, mine + xa], s_sa.at[k], s_pr.at[k], to_p).start()
        wait(xg.at[k, mine + xo], s_x2.at[k])
        send(xg.at[k, mine + xo], xg.at[k, mine + xo], s_sa.at[k], s_pr.at[k], to_p).start()

    def compute(k):
        wait(xg.at[k, pl.ds(0, NX)], s_pr.at[k])
        both = jnp.zeros((ROWS, 2 * units), F32)
        for slot in range(SECTIONS):
            sec = 2 * (slot % NX) + slot // NX
            both = both + jnp.dot(xg[k, slot], wgu[sec], preferred_element_type=F32)
        gate, up = both[:, :units], both[:, units:]
        hidden = (gate / (1.0 + jnp.exp(-gate)) * up).astype(BF16)
        for i in range(NX):
            part[k, theirs + i] = jnp.dot(hidden, wdn[2 * i + 1 - c], preferred_element_type=F32).astype(BF16)
        for i in range(NX):
            part[k, mine + i] = jnp.dot(hidden, wdn[2 * i + c], preferred_element_type=F32).astype(BF16)
            send(part.at[k, theirs + i], dbuf.at[k, i], s_sr.at[k], s_dr.at[k], to_p).start()

    def pair_sum(k, xx):
        return part[k, mine + xx].astype(F32) + dbuf[k, xx].astype(F32)

    def reduce_first(k):
        wait(dbuf.at[k], s_dr.at[k])
        part[k, mine + xo] = pair_sum(k, xo).astype(BF16)
        part[k, mine + xb] = pair_sum(k, xb).astype(BF16)
        send(part.at[k, mine + xo], r0.at[k], s_sr.at[k], s_r0.at[k], to_a).start()
        send(part.at[k, mine + xb], r1.at[k], s_sr.at[k], s_r1.at[k], to_b).start()

    def reduce_relay(k):
        wait(r0.at[k], s_r0.at[k])
        part[k, mine + xa] = (pair_sum(k, xa) + r0[k].astype(F32)).astype(BF16)
        send(part.at[k, mine + xa], r2.at[k], s_sr.at[k], s_r2.at[k], to_a).start()

    def reduce_last(k):
        wait(r1.at[k], s_r1.at[k])
        wait(r2.at[k], s_r2.at[k])
        total = (pair_sum(k, x) + (r1[k].astype(F32) + r2[k].astype(F32))).astype(BF16)
        zs[k] = total

        @pl.when(k == 0)
        def _():
            ret[0] = total

        @pl.when(k > 0)
        def _():
            d = distance(k)
            send(zs.at[k], ret.at[d], s_sz.at[1], s_ret.at[d], at_z((z - d + NZ) % NZ)).start()

    def turn(k, _):
        def stage(f, lag):
            @pl.when((k >= lag) & (k < CHUNKS + lag))
            def _():
                f(k - lag)

        @pl.when(k == 3)
        def _():
            g_copy.wait()
            u_copy.wait()
            for copy in d_copies:
                copy.wait()

        stage(gather_own, 0)
        stage(gather_relay, 1)
        stage(gather_rest, 2)
        stage(lambda q: reduce_first(reduce_order(q)), 7)
        stage(lambda q: reduce_relay(reduce_order(q)), 8)
        stage(lambda q: reduce_last(reduce_order(q)), 9)
        stage(lambda q: compute(reduce_order(q)), 6)
        return 0

    lax.fori_loop(0, LAST, turn, 0)

    for d in range(1, NZ):
        wait(ret.at[d], s_ret.at[d])
    for g in range(GROUPS):
        total = jnp.zeros((ROWS, feats), F32)
        for m in range(MEMBERS):
            total = total + ret[(MEMBERS * g + m - z + NZ) % NZ].astype(F32)
        merged[pl.ds(g * ROWS, ROWS), :] = total.astype(BF16)
    summed = merged[...]
    for i in range(NY):
        table = meta[i].T[:TOK]
        first = jnp.dot(oh[0, pl.ds(i * TOK, TOK), :], summed, preferred_element_type=F32)
        second = jnp.dot(oh[1, pl.ds(i * TOK, TOK), :], summed, preferred_element_type=F32)
        ysend[i] = (table[:, 0:1] * first + table[:, 1:2] * second).astype(BF16)
    for j in range(1, NY):
        yy = (y + j) % NY
        send(ysend.at[yy], yret.at[j], s_sy.at[2], s_yr.at[j], at_y(yy)).start()
    total = ysend[y].astype(F32)
    for j in range(1, NY):
        wait(yret.at[j], s_yr.at[j])
        total = total + yret[j].astype(F32)
    out[...] = total.astype(BF16)

    for k in range(CHUNKS):
        wait(xg.at[k, pl.ds(0, 7)], s_sa.at[k])
        wait(part.at[k, pl.ds(0, 7)], s_sr.at[k])
    wait(zs.at[pl.ds(0, 7)], s_sz.at[0])
    wait(zs.at[pl.ds(0, 7)], s_sz.at[1])
    wait(meta.at[pl.ds(0, 3)], s_sy.at[0])
    wait(tok.at[pl.ds(0, 3)], s_sy.at[1])
    wait(tok.at[pl.ds(0, 3)], s_sy.at[2])


def on_device(hidden_states, route_experts, route_weights, gate_weight, up_weight, down_weight):
    width = hidden_states.shape[1]
    units = gate_weight.shape[2]
    feats = width // SECTIONS
    dma = pltpu.SemaphoreType.DMA
    block = (ROWS, feats)
    return pl.pallas_call(
        kernel,
        out_shape=jax.ShapeDtypeStruct((TOK, feats), BF16),
        in_specs=[
            pl.BlockSpec(memory_space=pl.ANY),
            pl.BlockSpec(memory_space=pltpu.VMEM),
            pl.BlockSpec(memory_space=pltpu.VMEM),
            *[pl.BlockSpec(memory_space=pl.ANY)] * 3,
        ],
        out_specs=pl.BlockSpec(memory_space=pltpu.VMEM),
        scratch_shapes=[
            pltpu.VMEM((NY, TOK, feats), BF16),
            pltpu.VMEM((NY, 8, 128), F32),
            pltpu.VMEM((2, NY * TOK, GROUPS * ROWS), BF16),
            pltpu.VMEM((GROUPS * ROWS, feats), BF16),
            pltpu.VMEM((GROUPS, *block), BF16),
            pltpu.VMEM((SECTIONS, feats, 2 * units), BF16),
            pltpu.VMEM((SECTIONS, units, feats), BF16),
            pltpu.VMEM((CHUNKS, SECTIONS, *block), BF16),
            pltpu.VMEM((CHUNKS, SECTIONS, *block), BF16),
            pltpu.VMEM((CHUNKS, NX, *block), BF16),
            pltpu.VMEM((CHUNKS, *block), BF16),
            pltpu.VMEM((CHUNKS, *block), BF16),
            pltpu.VMEM((CHUNKS, *block), BF16),
            pltpu.VMEM((CHUNKS, *block), BF16),
            pltpu.VMEM((CHUNKS, *block), BF16),
            pltpu.VMEM((NY, TOK, feats), BF16),
            pltpu.VMEM((NY, TOK, feats), BF16),
            dma((3,)),
            dma((SECTIONS,)),
            *[dma((NY,))] * 3,
            *[dma((CHUNKS,))] * 10,
            dma((CHUNKS,)),
            dma((CHUNKS,)),
            dma((2,)),
            dma((3,)),
        ],
        compiler_params=pltpu.CompilerParams(
            collective_id=0, has_side_effects=True, vmem_limit_bytes=60 * 1024 * 1024
        ),
    )(
        hidden_states,
        route_experts.T,
        route_weights.T,
        gate_weight.reshape(SECTIONS, feats, units),
        up_weight.reshape(SECTIONS, feats, units),
        down_weight.reshape(units, width),
    )


def solution(mesh):
    return jax.shard_map(
        on_device,
        mesh=mesh,
        in_specs=(
            P("ep", None),
            P("ep", None),
            P("ep", None),
            P("ep", None, "section"),
            P("ep", None, "section"),
            P("ep", "section", None),
        ),
        out_specs=P("ep", "section"),
        check_vma=False,
    )
```

```python
import jax
import jax.numpy as jnp
from jax import lax
from jax.experimental import pallas as pl
from jax.experimental.pallas import tpu as pltpu
from jax.sharding import PartitionSpec as P

MESH = pl.DeviceIdType.MESH
BF16 = jnp.bfloat16
F32 = jnp.float32

NX, NY, NZ = 4, 4, 8
SECTIONS = 2 * NX
TOK = 48
CAP = 24
ROWS = NY * CAP
GROUPS = 2
MEMBERS = 4
FULL = 2
CHUNKS = NZ
LAST = CHUNKS + 8


def distance(k):
    return jnp.where(k % 2 == 1, (k + 1) // 2, (NZ - k // 2) % NZ)


def gather_order(a):
    return jnp.where(a == 0, 0, a + FULL)


def reduce_order(q):
    return jnp.where(q < 5, q + 3, jnp.where(q == 7, 0, q - 4))


def kernel(
    hid, experts, weights, wg, wu, wd, out,
    tok, meta, oh, merged, blk, wgu, wdn, xg, part, dbuf, r0, r1, r2, zs, ret, ysend, yret,
    s_loc, s_tok, s_wd, s_yt, s_ym, s_yr, s_zr, s_x0, s_x1, s_x2, s_pr, s_dr, s_r0, s_r1, s_r2, s_ret,
    s_sa, s_sr, s_sz, s_szf, s_sy, s_yf, s_syf,
):
    feats = tok.shape[-1]
    units = wdn.shape[1]
    s = lax.axis_index("section")
    ep = lax.axis_index("ep")
    c, x = s % 2, s // 2
    y, z = ep // NZ, ep % NZ
    step = 1 - 2 * c
    xa, xb, xo = (x + step + NX) % NX, (x - step + NX) % NX, (x + 2) % NX
    to_a = {"section": 2 * xa + c, "ep": ep}
    to_b = {"section": 2 * xb + c, "ep": ep}
    to_p = {"section": 2 * x + 1 - c, "ep": ep}
    mine, theirs = c * NX, (1 - c) * NX
    me = mine + x

    def at_y(yy):
        return {"section": s, "ep": yy * NZ + z}

    def at_z(zz):
        return {"section": s, "ep": y * NZ + zz}

    def send(src, dst, ssem, rsem, to):
        return pltpu.make_async_remote_copy(
            src_ref=src, dst_ref=dst, send_sem=ssem, recv_sem=rsem, device_id=to, device_id_type=MESH
        )

    def wait(ref, sem):
        pltpu.make_async_copy(ref, ref, sem).wait()

    tok_copies = []
    for i in range(NX):
        xx = (x + i) % NX
        start = pl.multiple_of((2 * xx + c) * feats, 128)
        tok_copies.append(pltpu.make_async_copy(hid.at[:, pl.ds(start, feats)], tok.at[xx, y], s_tok.at[i]))
        tok_copies[i].start()
    g_copy = pltpu.make_async_copy(wg, wgu.at[:, :, pl.ds(0, units)], s_loc.at[0])
    u_copy = pltpu.make_async_copy(wu, wgu.at[:, :, pl.ds(units, units)], s_loc.at[1])
    g_copy.start()
    u_copy.start()
    d_copies = [
        pltpu.make_async_copy(wd.at[:, pl.ds(i * feats, feats)], wdn.at[i], s_wd.at[i])
        for i in range(SECTIONS)
    ]
    for copy in d_copies:
        copy.start()

    meta[y] = jnp.zeros((8, 128), F32)
    meta[y, pl.ds(0, 2), pl.ds(0, TOK)] = weights[...]
    meta[y, pl.ds(2, 2), pl.ds(0, TOK)] = experts[...].astype(F32)

    barrier = pltpu.get_barrier_semaphore()
    peers = [at_y((y + j) % NY) for j in range(1, NY)]
    peers += [at_z((z + d) % NZ) for d in range(1, NZ)]
    peers += [to_a, to_b, to_p]
    for peer in peers:
        pl.semaphore_signal(barrier, inc=1, device_id=peer, device_id_type=MESH)
    pl.semaphore_wait(barrier, len(peers))

    for copy in tok_copies:
        copy.wait()
    for j in range(1, NY):
        to = at_y((y + j) % NY)
        send(meta.at[y], meta.at[y], s_sy.at[0], s_ym.at[j], to).start()
        send(tok.at[x, y], tok.at[x, y], s_sy.at[1], s_yt.at[j], to).start()
    for i in range(1, NX):
        xx = (x + i) % NX
        for j in range(1, NY):
            to = at_y((y + j) % NY)
            send(tok.at[xx, y], tok.at[xx, y], s_syf.at[i], s_yf.at[i], to).start()
    for j in range(1, NY):
        wait(meta.at[0], s_ym.at[j])

    lane = lax.broadcasted_iota(jnp.int32, (TOK, 128), 1).astype(F32)
    earlier = (
        lax.broadcasted_iota(jnp.int32, (TOK, TOK), 0) > lax.broadcasted_iota(jnp.int32, (TOK, TOK), 1)
    ).astype(F32).astype(BF16)
    slot_lane = lax.broadcasted_iota(jnp.int32, (TOK, GROUPS * ROWS), 1).astype(F32)
    first_expert = (GROUPS * y).astype(F32)
    for i in range(NY):
        table = meta[i].T[:TOK]
        named = [(table[:, 2 + n : 3 + n] == lane).astype(F32) for n in range(2)]
        before = jnp.dot(earlier, (named[0] + named[1]).astype(BF16), preferred_element_type=F32)
        for n in range(2):
            group = table[:, 2 + n : 3 + n] - first_expert
            place = group * ROWS + i * CAP + jnp.sum(named[n] * before, axis=1, keepdims=True)
            here = (group >= 0.0) & (group < float(GROUPS))
            place = jnp.where(here, place, -1.0)
            oh[n, pl.ds(i * TOK, TOK), :] = (place == slot_lane).astype(F32).astype(BF16)
    for j in range(1, NY):
        wait(tok.at[0, 0], s_yt.at[j])

    def pack(xx):
        rows = lax.dot_general(
            oh[0] + oh[1], tok[xx].reshape(NY * TOK, feats), (((0,), (0,)), ((), ())), preferred_element_type=F32
        ).astype(BF16)
        blk[0, xx] = rows[:ROWS]
        blk[1, xx] = rows[ROWS:]

    pack(x)
    xg[0, me] = blk[z // MEMBERS, x]
    for k in range(FULL + 1, CHUNKS):
        d = (k + 1) // 2 if k % 2 else NZ - k // 2
        zz = (z + d) % NZ
        send(blk.at[zz // MEMBERS, x], xg.at[k, me], s_sz.at[0], s_zr.at[k], at_z(zz)).start()

    def to_nearest(xx):
        for k in range(1, FULL + 1):
            zz = (z + (1 if k == 1 else NZ - 1)) % NZ
            send(blk.at[zz // MEMBERS, xx], xg.at[k, mine + xx], s_szf.at[0], s_zr.at[k], at_z(zz)).start()

    to_nearest(x)

    def spread(i):
        wait(tok.at[0, pl.ds(0, NY - 1)], s_yf.at[i])
        xx = (x + i) % NX
        pack(xx)
        to_nearest(xx)

    def gather_full(k):
        wait(xg.at[k, pl.ds(mine, NX)], s_zr.at[k])
        send(xg.at[k, pl.ds(mine, NX)], xg.at[k, pl.ds(mine, NX)], s_sa.at[k], s_pr.at[k], to_p).start()

    def gather_own(k):
        @pl.when(k > 0)
        def _():
            wait(xg.at[k, me], s_zr.at[k])

        send(xg.at[k, me], xg.at[k, me], s_sa.at[k], s_x0.at[k], to_a).start()
        send(xg.at[k, me], xg.at[k, me], s_sa.at[k], s_x1.at[k], to_b).start()
        send(xg.at[k, me], xg.at[k, me], s_sa.at[k], s_pr.at[k], to_p).start()

    def gather_relay(k):
        src = mine + xb
        wait(xg.at[k, src], s_x0.at[k])
        send(xg.at[k, src], xg.at[k, src], s_sa.at[k], s_x2.at[k], to_a).start()
        send(xg.at[k, src], xg.at[k, src], s_sa.at[k], s_pr.at[k], to_p).start()

    def gather_rest(k):
        wait(xg.at[k, mine + xa], s_x1.at[k])
        send(xg.at[k, mine + xa], xg.at[k, mine + xa], s_sa.at[k], s_pr.at[k], to_p).start()
        wait(xg.at[k, mine + xo], s_x2.at[k])
        send(xg.at[k, mine + xo], xg.at[k, mine + xo], s_sa.at[k], s_pr.at[k], to_p).start()

    def compute(k):
        wait(xg.at[k, pl.ds(0, NX)], s_pr.at[k])
        both = jnp.zeros((ROWS, 2 * units), F32)
        for slot in range(SECTIONS):
            sec = 2 * (slot % NX) + slot // NX
            both = both + jnp.dot(xg[k, slot], wgu[sec], preferred_element_type=F32)
        gate, up = both[:, :units], both[:, units:]
        hidden = (gate / (1.0 + jnp.exp(-gate)) * up).astype(BF16)
        for i in range(NX):
            part[k, theirs + i] = jnp.dot(hidden, wdn[2 * i + 1 - c], preferred_element_type=F32).astype(BF16)
        for i in range(NX):
            part[k, mine + i] = jnp.dot(hidden, wdn[2 * i + c], preferred_element_type=F32).astype(BF16)
            send(part.at[k, theirs + i], dbuf.at[k, i], s_sr.at[k], s_dr.at[k], to_p).start()

    def pair_sum(k, xx):
        return part[k, mine + xx].astype(F32) + dbuf[k, xx].astype(F32)

    def reduce_first(k):
        wait(dbuf.at[k], s_dr.at[k])
        part[k, mine + xo] = pair_sum(k, xo).astype(BF16)
        part[k, mine + xb] = pair_sum(k, xb).astype(BF16)
        send(part.at[k, mine + xo], r0.at[k], s_sr.at[k], s_r0.at[k], to_a).start()
        send(part.at[k, mine + xb], r1.at[k], s_sr.at[k], s_r1.at[k], to_b).start()

    def reduce_relay(k):
        wait(r0.at[k], s_r0.at[k])
        part[k, mine + xa] = (pair_sum(k, xa) + r0[k].astype(F32)).astype(BF16)
        send(part.at[k, mine + xa], r2.at[k], s_sr.at[k], s_r2.at[k], to_a).start()

    def reduce_last(k):
        wait(r1.at[k], s_r1.at[k])
        wait(r2.at[k], s_r2.at[k])
        total = (pair_sum(k, x) + (r1[k].astype(F32) + r2[k].astype(F32))).astype(BF16)
        zs[k] = total

        @pl.when(k == 0)
        def _():
            ret[0] = total

        @pl.when(k > 0)
        def _():
            d = distance(k)
            send(zs.at[k], ret.at[d], s_sz.at[1], s_ret.at[d], at_z((z - d + NZ) % NZ)).start()

    def turn(k, _):
        def stage(f, lag, count=CHUNKS):
            @pl.when((k >= lag) & (k < count + lag))
            def _():
                f(k - lag)

        @pl.when(k == 3)
        def _():
            g_copy.wait()
            u_copy.wait()
            for copy in d_copies:
                copy.wait()

        stage(lambda a: gather_relay(gather_order(a)), 2, CHUNKS - FULL)
        stage(lambda a: gather_rest(gather_order(a)), 3, CHUNKS - FULL)
        stage(lambda a: gather_own(gather_order(a)), 0, CHUNKS - FULL)
        stage(lambda i: spread(i + 1), 1, NX - 1)
        stage(lambda i: gather_full(i + 1), 8, FULL)
        stage(lambda q: reduce_first(reduce_order(q)), 6)
        stage(lambda q: reduce_relay(reduce_order(q)), 7)
        stage(lambda q: compute(reduce_order(q)), 4)
        stage(lambda q: reduce_last(reduce_order(q)), 8)
        return 0

    lax.fori_loop(0, LAST, turn, 0)

    for d in range(1, NZ):
        wait(ret.at[d], s_ret.at[d])
    for g in range(GROUPS):
        total = jnp.zeros((ROWS, feats), F32)
        for m in range(MEMBERS):
            total = total + ret[(MEMBERS * g + m - z + NZ) % NZ].astype(F32)
        merged[pl.ds(g * ROWS, ROWS), :] = total.astype(BF16)
    summed = merged[...]
    for i in range(NY):
        table = meta[i].T[:TOK]
        first = jnp.dot(oh[0, pl.ds(i * TOK, TOK), :], summed, preferred_element_type=F32)
        second = jnp.dot(oh[1, pl.ds(i * TOK, TOK), :], summed, preferred_element_type=F32)
        ysend[i] = (table[:, 0:1] * first + table[:, 1:2] * second).astype(BF16)
    for j in range(1, NY):
        yy = (y + j) % NY
        send(ysend.at[yy], yret.at[j], s_sy.at[2], s_yr.at[j], at_y(yy)).start()
    total = ysend[y].astype(F32)
    for j in range(1, NY):
        wait(yret.at[j], s_yr.at[j])
        total = total + yret[j].astype(F32)
    out[...] = total.astype(BF16)

    for k in range(CHUNKS):
        wait(xg.at[k, pl.ds(0, NX if 0 < k <= FULL else 7)], s_sa.at[k])
        wait(part.at[k, pl.ds(0, 7)], s_sr.at[k])
    wait(zs.at[pl.ds(0, CHUNKS - 1 - FULL)], s_sz.at[0])
    wait(xg.at[0], s_szf.at[0])
    for i in range(1, NX):
        wait(tok.at[0, pl.ds(0, 3)], s_syf.at[i])
    wait(zs.at[pl.ds(0, 7)], s_sz.at[1])
    wait(meta.at[pl.ds(0, 3)], s_sy.at[0])
    wait(tok.at[0, pl.ds(0, 3)], s_sy.at[1])
    wait(tok.at[0, pl.ds(0, 3)], s_sy.at[2])


def on_device(hidden_states, route_experts, route_weights, gate_weight, up_weight, down_weight):
    width = hidden_states.shape[1]
    units = gate_weight.shape[2]
    feats = width // SECTIONS
    dma = pltpu.SemaphoreType.DMA
    block = (ROWS, feats)
    return pl.pallas_call(
        kernel,
        out_shape=jax.ShapeDtypeStruct((TOK, feats), BF16),
        in_specs=[
            pl.BlockSpec(memory_space=pl.ANY),
            pl.BlockSpec(memory_space=pltpu.VMEM),
            pl.BlockSpec(memory_space=pltpu.VMEM),
            *[pl.BlockSpec(memory_space=pl.ANY)] * 3,
        ],
        out_specs=pl.BlockSpec(memory_space=pltpu.VMEM),
        scratch_shapes=[
            pltpu.VMEM((NX, NY, TOK, feats), BF16),
            pltpu.VMEM((NY, 8, 128), F32),
            pltpu.VMEM((2, NY * TOK, GROUPS * ROWS), BF16),
            pltpu.VMEM((GROUPS * ROWS, feats), BF16),
            pltpu.VMEM((GROUPS, NX, *block), BF16),
            pltpu.VMEM((SECTIONS, feats, 2 * units), BF16),
            pltpu.VMEM((SECTIONS, units, feats), BF16),
            pltpu.VMEM((CHUNKS, SECTIONS, *block), BF16),
            pltpu.VMEM((CHUNKS, SECTIONS, *block), BF16),
            pltpu.VMEM((CHUNKS, NX, *block), BF16),
            pltpu.VMEM((CHUNKS, *block), BF16),
            pltpu.VMEM((CHUNKS, *block), BF16),
            pltpu.VMEM((CHUNKS, *block), BF16),
            pltpu.VMEM((CHUNKS, *block), BF16),
            pltpu.VMEM((CHUNKS, *block), BF16),
            pltpu.VMEM((NY, TOK, feats), BF16),
            pltpu.VMEM((NY, TOK, feats), BF16),
            dma((2,)),
            dma((NX,)),
            dma((SECTIONS,)),
            *[dma((NY,))] * 3,
            *[dma((CHUNKS,))] * 10,
            dma((CHUNKS,)),
            dma((CHUNKS,)),
            dma((2,)),
            dma((1,)),
            dma((3,)),
            dma((NX,)),
            dma((NX,)),
        ],
        compiler_params=pltpu.CompilerParams(
            collective_id=0, has_side_effects=True, vmem_limit_bytes=60 * 1024 * 1024
        ),
    )(
        hidden_states,
        route_experts.T,
        route_weights.T,
        gate_weight.reshape(SECTIONS, feats, units),
        up_weight.reshape(SECTIONS, feats, units),
        down_weight.reshape(units, width),
    )


def solution(mesh):
    return jax.shard_map(
        on_device,
        mesh=mesh,
        in_specs=(
            P("ep", None),
            P("ep", None),
            P("ep", None),
            P("ep", None, "section"),
            P("ep", None, "section"),
            P("ep", "section", None),
        ),
        out_specs=P("ep", "section"),
        check_vma=False,
    )
```

```python
import jax
import jax.numpy as jnp
from jax import lax
from jax.experimental import pallas as pl
from jax.experimental.pallas import tpu as pltpu
from jax.sharding import PartitionSpec as P

MESH = pl.DeviceIdType.MESH
BF16 = jnp.bfloat16
F32 = jnp.float32

NX, NY, NZ = 4, 4, 8
SECTIONS = 2 * NX
TOK = 48
CAP = 24
ROWS = NY * CAP
GROUPS = 2
MEMBERS = 4
FULL = 2
CHUNKS = NZ
LAST = CHUNKS + 8


def distance(k):
    return jnp.where(k % 2 == 1, (k + 1) // 2, (NZ - k // 2) % NZ)


def gather_order(a):
    return jnp.where(a == 0, 0, a + FULL)


def reduce_order(q):
    return jnp.where(q < 5, q + 3, jnp.where(q == 7, 0, q - 4))


def kernel(
    hid, experts, weights, wg, wu, wd, out,
    tok, meta, oh, merged, blk, wgu, wdn, xg, part, dbuf, r0, r1, r2, zs, ret, ysend, yret,
    s_loc, s_tok, s_wd, s_yt, s_ym, s_yr, s_zr, s_x0, s_x1, s_x2, s_pr, s_dr, s_r0, s_r1, s_r2, s_ret,
    s_sa, s_sr, s_sz, s_szf, s_sy, s_yf, s_syf,
):
    feats = tok.shape[-1]
    units = wdn.shape[1]
    s = lax.axis_index("section")
    ep = lax.axis_index("ep")
    c, x = s % 2, s // 2
    y, z = ep // NZ, ep % NZ
    step = 1 - 2 * c
    xa, xb, xo = (x + step + NX) % NX, (x - step + NX) % NX, (x + 2) % NX
    to_a = {"section": 2 * xa + c, "ep": ep}
    to_b = {"section": 2 * xb + c, "ep": ep}
    to_p = {"section": 2 * x + 1 - c, "ep": ep}
    mine, theirs = c * NX, (1 - c) * NX
    me = mine + x

    def at_y(yy):
        return {"section": s, "ep": yy * NZ + z}

    def at_z(zz):
        return {"section": s, "ep": y * NZ + zz}

    def send(src, dst, ssem, rsem, to):
        return pltpu.make_async_remote_copy(
            src_ref=src, dst_ref=dst, send_sem=ssem, recv_sem=rsem, device_id=to, device_id_type=MESH
        )

    def wait(ref, sem):
        pltpu.make_async_copy(ref, ref, sem).wait()

    tok_copies = []
    for i in range(NX):
        xx = (x + i) % NX
        start = pl.multiple_of((2 * xx + c) * feats, 128)
        tok_copies.append(pltpu.make_async_copy(hid.at[:, pl.ds(start, feats)], tok.at[xx, y], s_tok.at[i]))
        tok_copies[i].start()
    g_copy = pltpu.make_async_copy(wg, wgu.at[:, :, pl.ds(0, units)], s_loc.at[0])
    u_copy = pltpu.make_async_copy(wu, wgu.at[:, :, pl.ds(units, units)], s_loc.at[1])
    g_copy.start()
    u_copy.start()
    d_copies = [
        pltpu.make_async_copy(wd.at[:, pl.ds(i * feats, feats)], wdn.at[i], s_wd.at[i])
        for i in range(SECTIONS)
    ]
    for copy in d_copies:
        copy.start()

    meta[y] = jnp.zeros((8, 128), F32)
    meta[y, pl.ds(0, 2), pl.ds(0, TOK)] = weights[...]
    meta[y, pl.ds(2, 2), pl.ds(0, TOK)] = experts[...].astype(F32)

    barrier = pltpu.get_barrier_semaphore()
    peers = [at_y((y + j) % NY) for j in range(1, NY)]
    peers += [at_z((z + d) % NZ) for d in range(1, NZ)]
    peers += [to_a, to_b, to_p]
    for peer in peers:
        pl.semaphore_signal(barrier, inc=1, device_id=peer, device_id_type=MESH)
    pl.semaphore_wait(barrier, len(peers))

    for copy in tok_copies:
        copy.wait()
    for j in (2, 1, 3):
        to = at_y((y + j) % NY)
        send(meta.at[y], meta.at[y], s_sy.at[0], s_ym.at[j], to).start()
        send(tok.at[x, y], tok.at[x, y], s_sy.at[1], s_yt.at[j], to).start()
    for i in range(1, NX):
        xx = (x + i) % NX
        for j in range(1, NY):
            to = at_y((y + j) % NY)
            send(tok.at[xx, y], tok.at[xx, y], s_syf.at[i], s_yf.at[i], to).start()
    for j in range(1, NY):
        wait(meta.at[0], s_ym.at[j])

    lane = lax.broadcasted_iota(jnp.int32, (TOK, 128), 1).astype(F32)
    earlier = (
        lax.broadcasted_iota(jnp.int32, (TOK, TOK), 0) > lax.broadcasted_iota(jnp.int32, (TOK, TOK), 1)
    ).astype(F32).astype(BF16)
    slot_lane = lax.broadcasted_iota(jnp.int32, (TOK, GROUPS * ROWS), 1).astype(F32)
    first_expert = (GROUPS * y).astype(F32)
    for i in range(NY):
        table = meta[i].T[:TOK]
        named = [(table[:, 2 + n : 3 + n] == lane).astype(F32) for n in range(2)]
        before = jnp.dot(earlier, (named[0] + named[1]).astype(BF16), preferred_element_type=F32)
        for n in range(2):
            group = table[:, 2 + n : 3 + n] - first_expert
            place = group * ROWS + i * CAP + jnp.sum(named[n] * before, axis=1, keepdims=True)
            here = (group >= 0.0) & (group < float(GROUPS))
            place = jnp.where(here, place, -1.0)
            oh[n, pl.ds(i * TOK, TOK), :] = (place == slot_lane).astype(F32).astype(BF16)
    for j in range(1, NY):
        wait(tok.at[0, 0], s_yt.at[j])

    def pack(xx):
        rows = lax.dot_general(
            oh[0] + oh[1], tok[xx].reshape(NY * TOK, feats), (((0,), (0,)), ((), ())), preferred_element_type=F32
        ).astype(BF16)
        blk[0, xx] = rows[:ROWS]
        blk[1, xx] = rows[ROWS:]

    pack(x)
    xg[0, me] = blk[z // MEMBERS, x]
    for k in range(FULL + 1, CHUNKS):
        d = (k + 1) // 2 if k % 2 else NZ - k // 2
        zz = (z + d) % NZ
        send(blk.at[zz // MEMBERS, x], xg.at[k, me], s_sz.at[0], s_zr.at[k], at_z(zz)).start()

    def to_nearest(xx):
        for k in range(1, FULL + 1):
            zz = (z + (1 if k == 1 else NZ - 1)) % NZ
            send(blk.at[zz // MEMBERS, xx], xg.at[k, mine + xx], s_szf.at[0], s_zr.at[k], at_z(zz)).start()

    to_nearest(x)

    def spread(i):
        wait(tok.at[0, pl.ds(0, NY - 1)], s_yf.at[i])
        xx = (x + i) % NX
        pack(xx)
        to_nearest(xx)

    def gather_full(k):
        wait(xg.at[k, pl.ds(mine, NX)], s_zr.at[k])
        send(xg.at[k, pl.ds(mine, NX)], xg.at[k, pl.ds(mine, NX)], s_sa.at[k], s_pr.at[k], to_p).start()

    def gather_own(k):
        @pl.when(k > 0)
        def _():
            wait(xg.at[k, me], s_zr.at[k])

        send(xg.at[k, me], xg.at[k, me], s_sa.at[k], s_x0.at[k], to_a).start()
        send(xg.at[k, me], xg.at[k, me], s_sa.at[k], s_x1.at[k], to_b).start()
        send(xg.at[k, me], xg.at[k, me], s_sa.at[k], s_pr.at[k], to_p).start()

    def gather_relay(k):
        src = mine + xb
        wait(xg.at[k, src], s_x0.at[k])
        send(xg.at[k, src], xg.at[k, src], s_sa.at[k], s_x2.at[k], to_a).start()
        send(xg.at[k, src], xg.at[k, src], s_sa.at[k], s_pr.at[k], to_p).start()

    def gather_rest(k):
        wait(xg.at[k, mine + xa], s_x1.at[k])
        send(xg.at[k, mine + xa], xg.at[k, mine + xa], s_sa.at[k], s_pr.at[k], to_p).start()
        wait(xg.at[k, mine + xo], s_x2.at[k])
        send(xg.at[k, mine + xo], xg.at[k, mine + xo], s_sa.at[k], s_pr.at[k], to_p).start()

    def compute(k):
        wait(xg.at[k, pl.ds(0, NX)], s_pr.at[k])
        both = jnp.zeros((ROWS, 2 * units), F32)
        for slot in range(SECTIONS):
            sec = 2 * (slot % NX) + slot // NX
            both = both + jnp.dot(xg[k, slot], wgu[sec], preferred_element_type=F32)
        gate, up = both[:, :units], both[:, units:]
        hidden = (gate / (1.0 + jnp.exp(-gate)) * up).astype(BF16)
        for i in range(NX):
            part[k, theirs + i] = jnp.dot(hidden, wdn[2 * i + 1 - c], preferred_element_type=F32).astype(BF16)
        for i in range(NX):
            part[k, mine + i] = jnp.dot(hidden, wdn[2 * i + c], preferred_element_type=F32).astype(BF16)
            send(part.at[k, theirs + i], dbuf.at[k, i], s_sr.at[k], s_dr.at[k], to_p).start()

    def pair_sum(k, xx):
        return part[k, mine + xx].astype(F32) + dbuf[k, xx].astype(F32)

    def reduce_first(k):
        wait(dbuf.at[k], s_dr.at[k])
        part[k, mine + xo] = pair_sum(k, xo).astype(BF16)
        part[k, mine + xb] = pair_sum(k, xb).astype(BF16)
        send(part.at[k, mine + xo], r0.at[k], s_sr.at[k], s_r0.at[k], to_a).start()
        send(part.at[k, mine + xb], r1.at[k], s_sr.at[k], s_r1.at[k], to_b).start()

    def reduce_relay(k):
        wait(r0.at[k], s_r0.at[k])
        part[k, mine + xa] = (pair_sum(k, xa) + r0[k].astype(F32)).astype(BF16)
        send(part.at[k, mine + xa], r2.at[k], s_sr.at[k], s_r2.at[k], to_a).start()

    def reduce_last(k):
        wait(r1.at[k], s_r1.at[k])
        wait(r2.at[k], s_r2.at[k])
        total = (pair_sum(k, x) + (r1[k].astype(F32) + r2[k].astype(F32))).astype(BF16)
        zs[k] = total

        @pl.when(k == 0)
        def _():
            ret[0] = total

        @pl.when(k > 0)
        def _():
            d = distance(k)
            send(zs.at[k], ret.at[d], s_sz.at[1], s_ret.at[d], at_z((z - d + NZ) % NZ)).start()

    def turn(k, _):
        def stage(f, lag, count=CHUNKS):
            @pl.when((k >= lag) & (k < count + lag))
            def _():
                f(k - lag)

        @pl.when(k == 3)
        def _():
            g_copy.wait()
            u_copy.wait()
            for copy in d_copies:
                copy.wait()

        stage(lambda a: gather_relay(gather_order(a)), 2, CHUNKS - FULL)
        stage(lambda a: gather_rest(gather_order(a)), 3, CHUNKS - FULL)
        stage(lambda a: gather_own(gather_order(a)), 0, CHUNKS - FULL)
        stage(lambda i: spread(i + 1), 1, NX - 1)
        stage(lambda i: gather_full(i + 1), 8, FULL)
        stage(lambda q: reduce_first(reduce_order(q)), 6)
        stage(lambda q: reduce_relay(reduce_order(q)), 7)
        stage(lambda q: compute(reduce_order(q)), 4)
        stage(lambda q: reduce_last(reduce_order(q)), 8)
        return 0

    lax.fori_loop(0, LAST, turn, 0)

    for d in range(1, NZ):
        wait(ret.at[d], s_ret.at[d])
    for g in range(GROUPS):
        total = jnp.zeros((ROWS, feats), F32)
        for m in range(MEMBERS):
            total = total + ret[(MEMBERS * g + m - z + NZ) % NZ].astype(F32)
        merged[pl.ds(g * ROWS, ROWS), :] = total.astype(BF16)
    summed = merged[...]
    for i in range(NY):
        table = meta[i].T[:TOK]
        first = jnp.dot(oh[0, pl.ds(i * TOK, TOK), :], summed, preferred_element_type=F32)
        second = jnp.dot(oh[1, pl.ds(i * TOK, TOK), :], summed, preferred_element_type=F32)
        ysend[i] = (table[:, 0:1] * first + table[:, 1:2] * second).astype(BF16)
    for j in (2, 1, 3):
        yy = (y + j) % NY
        send(ysend.at[yy], yret.at[j], s_sy.at[2], s_yr.at[j], at_y(yy)).start()
    total = ysend[y].astype(F32)
    for j in range(1, NY):
        wait(yret.at[j], s_yr.at[j])
        total = total + yret[j].astype(F32)
    out[...] = total.astype(BF16)

    for k in range(CHUNKS):
        wait(xg.at[k, pl.ds(0, NX if 0 < k <= FULL else 7)], s_sa.at[k])
        wait(part.at[k, pl.ds(0, 7)], s_sr.at[k])
    wait(zs.at[pl.ds(0, CHUNKS - 1 - FULL)], s_sz.at[0])
    wait(xg.at[0], s_szf.at[0])
    for i in range(1, NX):
        wait(tok.at[0, pl.ds(0, 3)], s_syf.at[i])
    wait(zs.at[pl.ds(0, 7)], s_sz.at[1])
    wait(meta.at[pl.ds(0, 3)], s_sy.at[0])
    wait(tok.at[0, pl.ds(0, 3)], s_sy.at[1])
    wait(tok.at[0, pl.ds(0, 3)], s_sy.at[2])


def on_device(hidden_states, route_experts, route_weights, gate_weight, up_weight, down_weight):
    width = hidden_states.shape[1]
    units = gate_weight.shape[2]
    feats = width // SECTIONS
    dma = pltpu.SemaphoreType.DMA
    block = (ROWS, feats)
    return pl.pallas_call(
        kernel,
        out_shape=jax.ShapeDtypeStruct((TOK, feats), BF16),
        in_specs=[
            pl.BlockSpec(memory_space=pl.ANY),
            pl.BlockSpec(memory_space=pltpu.VMEM),
            pl.BlockSpec(memory_space=pltpu.VMEM),
            *[pl.BlockSpec(memory_space=pl.ANY)] * 3,
        ],
        out_specs=pl.BlockSpec(memory_space=pltpu.VMEM),
        scratch_shapes=[
            pltpu.VMEM((NX, NY, TOK, feats), BF16),
            pltpu.VMEM((NY, 8, 128), F32),
            pltpu.VMEM((2, NY * TOK, GROUPS * ROWS), BF16),
            pltpu.VMEM((GROUPS * ROWS, feats), BF16),
            pltpu.VMEM((GROUPS, NX, *block), BF16),
            pltpu.VMEM((SECTIONS, feats, 2 * units), BF16),
            pltpu.VMEM((SECTIONS, units, feats), BF16),
            pltpu.VMEM((CHUNKS, SECTIONS, *block), BF16),
            pltpu.VMEM((CHUNKS, SECTIONS, *block), BF16),
            pltpu.VMEM((CHUNKS, NX, *block), BF16),
            pltpu.VMEM((CHUNKS, *block), BF16),
            pltpu.VMEM((CHUNKS, *block), BF16),
            pltpu.VMEM((CHUNKS, *block), BF16),
            pltpu.VMEM((CHUNKS, *block), BF16),
            pltpu.VMEM((CHUNKS, *block), BF16),
            pltpu.VMEM((NY, TOK, feats), BF16),
            pltpu.VMEM((NY, TOK, feats), BF16),
            dma((2,)),
            dma((NX,)),
            dma((SECTIONS,)),
            *[dma((NY,))] * 3,
            *[dma((CHUNKS,))] * 10,
            dma((CHUNKS,)),
            dma((CHUNKS,)),
            dma((2,)),
            dma((1,)),
            dma((3,)),
            dma((NX,)),
            dma((NX,)),
        ],
        compiler_params=pltpu.CompilerParams(
            collective_id=0, has_side_effects=True, vmem_limit_bytes=60 * 1024 * 1024
        ),
    )(
        hidden_states,
        route_experts.T,
        route_weights.T,
        gate_weight.reshape(SECTIONS, feats, units),
        up_weight.reshape(SECTIONS, feats, units),
        down_weight.reshape(units, width),
    )


def solution(mesh):
    return jax.shard_map(
        on_device,
        mesh=mesh,
        in_specs=(
            P("ep", None),
            P("ep", None),
            P("ep", None),
            P("ep", None, "section"),
            P("ep", None, "section"),
            P("ep", "section", None),
        ),
        out_specs=P("ep", "section"),
        check_vma=False,
    )
```
